128 devices in a mesh: ep: 4 (over y), fsdp: 32 (over z, x, core).
Axes of the slice: x: 4, y: 4, z: 4, core: 2. Of those that a mesh axis runs over, the one named last changes fastest.
Arguments:
- train_gate: float32 [128, 2048, 768], P('ep', 'fsdp'), may hold values from -0.25 to 0.25
- other_gate: bfloat16 [128, 2048, 768], P('ep', 'fsdp'), may hold values from -0.0625 to 0.0625
- train_up: float32 [128, 2048, 768], P('ep', 'fsdp'), may hold values from -0.25 to 0.25
- other_up: bfloat16 [128, 2048, 768], P('ep', 'fsdp'), may hold values from -0.0625 to 0.0625
- router_weight: float32 [2048, 128], P('fsdp', 'ep'), may hold values from -0.125 to 0.125
- router_gain: float32 [2048], P('fsdp'), may hold values from 0.25 to 1.75
Outputs:
- ready_gate: bfloat16 [128, 2048, 768], P(('ep', 'fsdp'))
- ready_up: bfloat16 [128, 2048, 768], P(('ep', 'fsdp'))
- scale_gate: float32 [128, 768], P(('ep', 'fsdp'))
- scale_up: float32 [128, 768], P(('ep', 'fsdp'))
- serve_router: bfloat16 [2048, 128], replicated
The draws below stay inside these ranges and needn't reach their ends.
All inputs are finite; a program needn't handle non-finite values. Where the reference program divides by a largest or mean magnitude, that divisor is 1e-20 or more.
Results may differ from the reference program's by a relative error of at most 0.013.
Values may be sent and summed in bfloat16 or wider, within the bound.
No kernel may reach another device: no remote copies, remote signals or barrier semaphores. Data moves between devices by JAX's collectives and lax.ppermute only.
A program may use at most 128 MiB of HBM per device.

```python
import jax
import jax.numpy as jnp

EXPERTS = 128
D_MODEL = 2048
D_EXPERT = 768


def raised(drawn, key, source, target, shards_of, factor):
    def block_of(dim):
        return (jnp.arange(drawn.shape[dim]) // (drawn.shape[dim] // shards_of)).reshape((-1,) + (1,) * (drawn.ndim - 1 - dim))

    first = jax.random.permutation(key, shards_of)[block_of(target)]
    second = (block_of(target) + shards_of // 2) % shards_of
    return jnp.where((block_of(source) == first) | (block_of(source) == second), factor * drawn, drawn)


def steps_of(own_key, shape, shards, smallest, top_value):
    gain, own = 1.0, jax.random.fold_in(own_key, 6)
    for position, parts in shards:
        steps = jnp.exp(jax.random.uniform(jax.random.fold_in(own, position), (parts,), jnp.float32, smallest / len(shards), top_value / len(shards)))
        gain = gain * jnp.repeat(steps, shape[position] // parts).reshape([-1 if axis == position else 1 for axis in range(len(shape))])
    return gain


def gaussian(rng, shape, scale, most, pieces=(), kind=jnp.bfloat16):
    loudness = steps_of(rng, shape, pieces, -0.22, 0.18) if pieces else 1.0
    values = jax.random.normal(rng, shape, jnp.float32) * scale * loudness
    return jnp.minimum(jnp.maximum(values, -most), most).astype(kind)


def noise_with(rng, shape, width, most, shards, heavy, held_as=jnp.bfloat16):
    array = width * jax.random.normal(rng, shape, jnp.float32)
    if shards:
        array = array * steps_of(rng, shape, shards, -0.22, 0.18)
    return jnp.clip(raised(array, jax.random.fold_in(rng, 3), *heavy), -most, most).astype(held_as)


def setup_inputs(seed: int = 0) -> dict:
    arg_keys = jax.random.split(jax.random.key(seed), 7)
    return {
        "train_gate": noise_with(arg_keys[0], (EXPERTS, D_MODEL, D_EXPERT), D_MODEL ** -0.5, 0.25, ((0, 4), (1, 32)), (1, 2, 32, 2.75), jnp.float32),
        "other_gate": gaussian(arg_keys[1], (EXPERTS, D_MODEL, D_EXPERT), (D_MODEL * 4) ** -0.5, 0.0625, ((0, 4), (1, 32))),
        "train_up": noise_with(arg_keys[2], (EXPERTS, D_MODEL, D_EXPERT), D_MODEL ** -0.5, 0.25, ((0, 4), (1, 32)), (1, 2, 32, 2.75), jnp.float32),
        "other_up": gaussian(arg_keys[3], (EXPERTS, D_MODEL, D_EXPERT), (D_MODEL * 4) ** -0.5, 0.0625, ((0, 4), (1, 32))),
        "router_weight": gaussian(arg_keys[4], (D_MODEL, EXPERTS), D_MODEL ** -0.5, 0.125, ((0, 32), (1, 4)), jnp.float32),
        "router_gain": jnp.clip(1.0 + 0.15 * jax.random.normal(arg_keys[5], (D_MODEL,), jnp.float32), 0.25, 1.75),
    }


def reference(train_gate, other_gate, train_up, other_up, router_weight, router_gain):
    latest_gate = train_gate + other_gate.astype(jnp.float32)
    latest_up = train_up + other_up.astype(jnp.float32)
    scale_gate = jnp.sum(jnp.abs(latest_gate), axis=1) / D_MODEL
    ready_gate = (latest_gate / jnp.expand_dims(scale_gate, 1)).astype(jnp.bfloat16)
    scale_up = jnp.sum(jnp.abs(latest_up), axis=1) / D_MODEL
    ready_up = (latest_up / jnp.expand_dims(scale_up, 1)).astype(jnp.bfloat16)
    serve_router = (router_weight * router_gain[:, None]).astype(jnp.bfloat16)
    return ready_gate, ready_up, scale_gate, scale_up, serve_router
```

```python
import jax
import jax.numpy as jnp
from jax import lax
from jax.sharding import PartitionSpec as P

D_MODEL = 2048


def regrouped(train, other):
    latest = (train + other.astype(jnp.float32)).astype(jnp.bfloat16)
    return lax.all_to_all(latest, "fsdp", split_axis=0, concat_axis=1, tiled=True)


def readied(latest):
    wide = latest.astype(jnp.float32)
    scale = jnp.sum(jnp.abs(wide), axis=1) / D_MODEL
    ready = (wide / jnp.expand_dims(scale, 1)).astype(jnp.bfloat16)
    return ready, scale


def shards(train_gate, other_gate, train_up, other_up, router_weight, router_gain):
    gate = regrouped(train_gate, other_gate)
    up = regrouped(train_up, other_up)
    ready_gate, scale_gate = readied(gate)
    ready_up, scale_up = readied(up)
    part_router = (router_weight * router_gain[:, None]).astype(jnp.bfloat16)
    row_router = lax.all_gather(part_router, "fsdp", axis=0, tiled=True)
    serve_router = lax.all_gather(row_router, "ep", axis=1, tiled=True)
    return (ready_gate, ready_up, scale_gate, scale_up, serve_router)


def solution(mesh):
    placed = (
        P("ep", "fsdp", None),
        P("ep", "fsdp", None),
        P("ep", "fsdp", None),
        P("ep", "fsdp", None),
        P("fsdp", "ep"),
        P("fsdp"),
    )
    return jax.shard_map(
        shards,
        mesh=mesh,
        in_specs=placed,
        out_specs=(
            P(("ep", "fsdp"), None, None),
            P(("ep", "fsdp"), None, None),
            P(("ep", "fsdp"), None),
            P(("ep", "fsdp"), None),
            P(),
        ),
        check_vma=False,
    )
```

```python
import jax
import jax.numpy as jnp
from jax import lax
from jax.experimental import pallas as pl
from jax.experimental.pallas import tpu as pltpu
from jax.sharding import PartitionSpec as P


D_MODEL = 2048
D_EXPERT = 768
ROWS = 64
SIDE = 4
CORES = 2
PEERS = SIDE * SIDE * CORES


PIECE = jax.ShapeDtypeStruct((SIDE, ROWS, D_EXPERT), jnp.bfloat16)
HELD = jax.ShapeDtypeStruct((PEERS, ROWS, D_EXPERT), jnp.bfloat16)


def member(z, x, c):
    return (z % SIDE) * SIDE * CORES + (x % SIDE) * CORES + c


def moved(array, dz, dx, dc):
    pairs = [
        (member(z, x, c), member(z + dz, x + dx, c ^ dc))
        for z in range(SIDE)
        for x in range(SIDE)
        for c in range(CORES)
    ]
    return lax.ppermute(array, "fsdp", pairs)


def spot(at):
    place = at[0]
    return place >> 3, (place >> 1) & 3, place & 1


def latest_of(train, other):
    return (train + other.astype(jnp.float32)).astype(jnp.bfloat16)


def part_kernel(at, train_x, other_x, train_z, other_z, *outs):
    for n in range(len(outs) // 2):

        @pl.when(pl.program_id(0) == n)
        def _(n=n):
            outs[2 * n][...] = latest_of(train_x[...], other_x[...])
            outs[2 * n + 1][...] = latest_of(train_z[...], other_z[...])


def parts_of(at, train, other, steps):
    shape = (SIDE, SIDE, CORES, ROWS, D_EXPERT)
    train, other = train.reshape(shape), other.reshape(shape)
    base, stride = steps[0], steps[1] - steps[0]

    def for_x(n, at):
        _, x, c = spot(at)
        return 0, (x + base + stride * n) & 3, c, 0, 0

    def for_z(n, at):
        z, _, c = spot(at)
        return (z + base + stride * n) & 3, 0, 1 - c, 0, 0

    cut_x = pl.BlockSpec((SIDE, None, None, ROWS, D_EXPERT), for_x)
    cut_z = pl.BlockSpec((None, SIDE, None, ROWS, D_EXPERT), for_z)
    whole = pl.BlockSpec(PIECE.shape, lambda n, at: (0, 0, 0))
    outs = 2 * len(steps)
    parts = pl.pallas_call(
        part_kernel,
        grid_spec=pltpu.PrefetchScalarGridSpec(
            num_scalar_prefetch=1,
            grid=(len(steps),),
            in_specs=[cut_x, cut_x, cut_z, cut_z],
            out_specs=[whole] * outs,
        ),
        out_shape=[PIECE] * outs,
    )(at, train, other, train, other)
    return {k: parts[2 * n] for n, k in enumerate(steps)}, {
        k: parts[2 * n + 1] for n, k in enumerate(steps)
    }


def regroup_kernel(at, *refs):
    over_x, over_z, outs = refs[:4], refs[4:8], refs[8:15]
    held, in_sems, out_sems = refs[15:]
    z, x, _ = spot(at)
    loads, stores = [], []
    for place, sources, steps in ((z, over_x, (1, 3, 2)), (x, over_z, (1, 3, 2, 0))):
        for k in steps:
            n = len(stores)
            loads.append(
                [
                    pltpu.make_async_copy(ref.at[(place + k) & 3], held.at[n, j], in_sems.at[n, j])
                    for j, ref in enumerate(sources)
                ]
            )
            stores.append(pltpu.make_async_copy(held.at[n], outs[n], out_sems.at[n]))
    for load in loads:
        for copy in load:
            copy.start()
    for load, store in zip(loads, stores):
        for copy in load:
            copy.wait()
        store.start()
    for store in stores:
        store.wait()


def regrouped(at, over_x, over_z):
    hbm = pl.BlockSpec(memory_space=pltpu.HBM)
    outs = pl.pallas_call(
        regroup_kernel,
        in_specs=[pl.BlockSpec(memory_space=pltpu.SMEM)] + [hbm] * 8,
        out_specs=[hbm] * 7,
        out_shape=[PIECE] * 7,
        scratch_shapes=[
            pltpu.VMEM((7, *PIECE.shape), PIECE.dtype),
            pltpu.SemaphoreType.DMA((7, SIDE)),
            pltpu.SemaphoreType.DMA((7,)),
        ],
    )(at, *over_x, *over_z)
    return dict(zip((1, 3, 2), outs[:3])), dict(zip((1, 3, 2, 0), outs[3:]))


def ready_of(loads, slot, ready, scale, held, in_sems, out_sems):
    copies = [
        (pltpu.make_async_copy(ref, held.at[pl.ds(first, count)], in_sems.at[n]), first, count)
        for n, (ref, first, count) in enumerate(loads)
    ]
    for copy, _, _ in copies:
        copy.start()

    def added(n, total):
        for r in range(0, ROWS, 16):
            rows = jnp.abs(held[n, pl.ds(r, 16)].astype(jnp.float32))
            total = total + rows[:8] + rows[8:]
        return total

    total = jnp.zeros((8, D_EXPERT), jnp.float32)
    for copy, first, count in copies:
        copy.wait()
        total = lax.fori_loop(first, first + count, added, total)
    mean = jnp.sum(total, axis=0, keepdims=True) / D_MODEL
    scale[...] = mean
    factor = jnp.broadcast_to(1.0 / mean, (16, D_EXPERT))

    def out_copy(n):
        to = pl.ds(pl.multiple_of(slot(n) * ROWS, ROWS), ROWS)
        return pltpu.make_async_copy(held.at[n], ready.at[to], out_sems.at[n])

    def scaled(n, carry):
        for r in range(0, ROWS, 16):
            rows = pl.ds(r, 16)
            held[n, rows] = (held[n, rows].astype(jnp.float32) * factor).astype(jnp.bfloat16)
        out_copy(n).start()
        return carry

    def awaited(n, carry):
        out_copy(n).wait()
        return carry

    lax.fori_loop(0, PEERS, scaled, 0)
    lax.fori_loop(0, PEERS, awaited, 0)


def plain_kernel(held_in, *refs):
    loads = [(held_in.at[pl.ds(n, SIDE)], n, SIDE) for n in range(0, PEERS, SIDE)]
    ready_of(loads, lambda n: n, *refs)


def pieces_kernel(at, *refs):
    z, x, c = spot(at)
    own, pieces, rest = refs[:4], refs[4:11], refs[11:]
    loads = [(ref.at[pl.ds(z, 1)], n, 1) for n, ref in enumerate(own)]
    loads += [(ref, SIDE * (n + 1), SIDE) for n, ref in enumerate(pieces)]

    def slot(n):
        far, near = (n >> 2) & 3, n & 3
        by_x = n >> 4
        back_z = (z - jnp.where(by_x == 0, far, near)) & 3
        back_x = (x - jnp.where(by_x == 0, near, far)) & 3
        return back_z * 8 + back_x * 2 + ((c + by_x) & 1)

    ready_of(loads, slot, *rest)


def readied(kernel, operands, loads, at=None):
    hbm = pl.BlockSpec(memory_space=pltpu.HBM)
    first = [] if at is None else [pl.BlockSpec(memory_space=pltpu.SMEM)]
    ready, scale = pl.pallas_call(
        kernel,
        in_specs=first + [hbm] * len(operands),
        out_specs=(hbm, pl.BlockSpec(memory_space=pltpu.VMEM)),
        out_shape=(
            jax.ShapeDtypeStruct((D_MODEL, D_EXPERT), jnp.bfloat16),
            jax.ShapeDtypeStruct((1, D_EXPERT), jnp.float32),
        ),
        scratch_shapes=[
            pltpu.VMEM(HELD.shape, HELD.dtype),
            pltpu.SemaphoreType.DMA((loads,)),
            pltpu.SemaphoreType.DMA((PEERS,)),
        ],
    )(*([] if at is None else [at]), *operands)
    return ready[None], scale


def sent_to_all(array, axis):
    peers = lax.axis_size(axis)
    return lax.all_to_all(
        jnp.broadcast_to(array[None], (peers, *array.shape)), axis, 0, 0, tiled=True
    )


def shards(train_gate, other_gate, train_up, other_up, router_weight, router_gain):
    at = lax.axis_index("fsdp").reshape(1)
    early_x, early_z = parts_of(at, train_up, other_up, (1, 3))
    late_x, late_z = parts_of(at, train_up, other_up, (2, 0))
    part_x, part_z = early_x | late_x, early_z | late_z
    over_x, over_z = [part_x[0]], [part_z[0]]
    for k in (1, 2, 3):
        over_x.append(moved(part_x[k], 0, k, 0))
        over_z.append(moved(part_z[k], k, 0, 0))
    gate = latest_of(train_gate, other_gate)
    gate = lax.all_to_all(gate, "fsdp", split_axis=0, concat_axis=0, tiled=True)
    next_z, next_x = regrouped(at, over_x, over_z)
    then_z, then_x = [], []
    for k in range(SIDE):
        then_x.append(moved(next_x[k], 0, k, 1))
        if k:
            then_z.append(moved(next_z[k], k, 0, 0))
    part_router = (router_weight * router_gain[:, None]).astype(jnp.bfloat16)
    row_router = sent_to_all(part_router, "fsdp").reshape(D_MODEL, -1)
    columns = sent_to_all(row_router, "ep")
    serve_router = jnp.moveaxis(columns, 0, 1).reshape(D_MODEL, -1)
    ready_gate, scale_gate = readied(plain_kernel, [gate], 8)
    up = [*over_x, *then_z, *then_x]
    ready_up, scale_up = readied(pieces_kernel, up, 11, at=at)
    return (ready_gate, ready_up, scale_gate, scale_up, serve_router)


def solution(mesh):
    placed = (
        P("ep", "fsdp", None),
        P("ep", "fsdp", None),
        P("ep", "fsdp", None),
        P("ep", "fsdp", None),
        P("fsdp", "ep"),
        P("fsdp"),
    )
    return jax.shard_map(
        shards,
        mesh=mesh,
        in_specs=placed,
        out_specs=(
            P(("ep", "fsdp"), None, None),
            P(("ep", "fsdp"), None, None),
            P(("ep", "fsdp"), None),
            P(("ep", "fsdp"), None),
            P(),
        ),
        check_vma=False,
    )
```

```python
import jax
import jax.numpy as jnp
from jax import lax
from jax.experimental import pallas as pl
from jax.experimental.pallas import tpu as pltpu
from jax.sharding import PartitionSpec as P


D_MODEL = 2048
D_EXPERT = 768
ROWS = 64
SIDE = 4
CORES = 2
PEERS = SIDE * SIDE * CORES
TALL = 16
LANES = 128
TILED = ROWS * D_EXPERT // LANES


PIECE = jax.ShapeDtypeStruct((SIDE, ROWS, D_EXPERT), jnp.bfloat16)


def member(z, x, c):
    return (z % SIDE) * SIDE * CORES + (x % SIDE) * CORES + c


def moved(array, dz, dx, dc):
    pairs = [
        (member(z, x, c), member(z + dz, x + dx, c ^ dc))
        for z in range(SIDE)
        for x in range(SIDE)
        for c in range(CORES)
    ]
    return lax.ppermute(array, "fsdp", pairs)


def spot(at):
    place = at[0]
    return place >> 3, (place >> 1) & 3, place & 1


def latest_of(train, other):
    return (train + other.astype(jnp.float32)).astype(jnp.bfloat16)


def part_kernel(at, train_x, other_x, train_z, other_z, *outs):
    for n in range(len(outs) // 2):

        @pl.when(pl.program_id(0) == n)
        def _(n=n):
            outs[2 * n][...] = latest_of(train_x[...], other_x[...])
            outs[2 * n + 1][...] = latest_of(train_z[...], other_z[...])


def parts_of(at, train, other, steps):
    shape = (SIDE, SIDE, CORES, ROWS, D_EXPERT)
    train, other = train.reshape(shape), other.reshape(shape)
    base, stride = steps[0], steps[1] - steps[0]

    def for_x(n, at):
        _, x, c = spot(at)
        return 0, (x + base + stride * n) & 3, c, 0, 0

    def for_z(n, at):
        z, _, c = spot(at)
        return (z + base + stride * n) & 3, 0, 1 - c, 0, 0

    cut_x = pl.BlockSpec((SIDE, None, None, ROWS, D_EXPERT), for_x)
    cut_z = pl.BlockSpec((None, SIDE, None, ROWS, D_EXPERT), for_z)
    whole = pl.BlockSpec(PIECE.shape, lambda n, at: (0, 0, 0))
    outs = 2 * len(steps)
    parts = pl.pallas_call(
        part_kernel,
        grid_spec=pltpu.PrefetchScalarGridSpec(
            num_scalar_prefetch=1,
            grid=(len(steps),),
            in_specs=[cut_x, cut_x, cut_z, cut_z],
            out_specs=[whole] * outs,
        ),
        out_shape=[PIECE] * outs,
    )(at, train, other, train, other)
    return {k: parts[2 * n] for n, k in enumerate(steps)}, {
        k: parts[2 * n + 1] for n, k in enumerate(steps)
    }


def tiles_of(rows):
    return [(r, t) for r in range(0, rows, TALL) for t in range(0, D_EXPERT, LANES)]


def gate_kernel(train, other, weight, gain, sent):
    router = weight[...] * gain[...]
    router = jnp.concatenate([router[:TALL], router[TALL:]], axis=1).astype(jnp.bfloat16)
    for e in range(sent.shape[0]):
        for n, (r, t) in enumerate(tiles_of(ROWS)):
            cut = e, pl.ds(r, TALL), pl.ds(t, LANES)
            sent[e, pl.ds(n * TALL, TALL)] = latest_of(train[cut], other[cut])
        sent[e, pl.ds(TILED, TALL)] = router


def gate_update(train, other, weight, gain):
    each = 8
    cut = pl.BlockSpec((each, ROWS, D_EXPERT), lambda n: (n, 0, 0))
    return pl.pallas_call(
        gate_kernel,
        grid=(PEERS // each,),
        in_specs=[
            cut,
            cut,
            pl.BlockSpec((2 * TALL, ROWS), lambda n: (0, 0)),
            pl.BlockSpec((1, ROWS), lambda n: (0, 0)),
        ],
        out_specs=pl.BlockSpec((each, TILED + TALL, LANES), lambda n: (n, 0, 0)),
        out_shape=jax.ShapeDtypeStruct((PEERS, TILED + TALL, LANES), jnp.bfloat16),
        name="gate_update",
    )(train, other, weight.T, gain.reshape(1, ROWS))


def regroup_kernel(at, *refs):
    over_x, over_z, outs = refs[:4], refs[4:8], refs[8:15]
    held, in_sems, out_sems = refs[15:]
    z, x, _ = spot(at)
    loads, stores = [], []
    for place, sources, steps in ((z, over_x, (1, 3, 2)), (x, over_z, (1, 3, 2, 0))):
        for k in steps:
            n = len(stores)
            loads.append(
                [
                    pltpu.make_async_copy(ref.at[(place + k) & 3], held.at[n, j], in_sems.at[n, j])
                    for j, ref in enumerate(sources)
                ]
            )
            stores.append(pltpu.make_async_copy(held.at[n], outs[n], out_sems.at[n]))
    for load in loads:
        for copy in load:
            copy.start()
    for load, store in zip(loads, stores):
        for copy in load:
            copy.wait()
        store.start()
    for store in stores:
        store.wait()


def regrouped(at, over_x, over_z):
    hbm = pl.BlockSpec(memory_space=pltpu.HBM)
    outs = pl.pallas_call(
        regroup_kernel,
        in_specs=[pl.BlockSpec(memory_space=pltpu.SMEM)] + [hbm] * 8,
        out_specs=[hbm] * 7,
        out_shape=[PIECE] * 7,
        scratch_shapes=[
            pltpu.VMEM((7, *PIECE.shape), PIECE.dtype),
            pltpu.SemaphoreType.DMA((7, SIDE)),
            pltpu.SemaphoreType.DMA((7,)),
        ],
    )(at, *over_x, *over_z)
    return dict(zip((1, 3, 2), outs[:3])), dict(zip((1, 3, 2, 0), outs[3:]))


def out_copies(ready, held, slot, sems):
    def out_copy(n):
        to = pl.ds(pl.multiple_of(slot(n) * ROWS, ROWS), ROWS)
        return pltpu.make_async_copy(held.at[n], ready.at[to], sems.at[n])

    return out_copy


def in_copies(loads, held, sems):
    copies = [
        (pltpu.make_async_copy(ref, held.at[pl.ds(first, count)], sems.at[n]), first, count)
        for n, (ref, first, count) in enumerate(loads)
    ]
    for copy, _, _ in copies:
        copy.start()
    return copies


def for_each(body):
    def step(n, carry):
        body(n)
        return carry

    lax.fori_loop(0, PEERS, step, 0)


def gate_ready_kernel(got, ready, scale, tiled, held, in_sems, out_sems):
    loads = [(got.at[pl.ds(n, SIDE)], n, SIDE) for n in range(0, PEERS, SIDE)]
    tiles = tiles_of(ROWS)

    def added(n, totals):
        totals = list(totals)
        for m, (r, t) in enumerate(tiles):
            rows = jnp.abs(tiled[n, pl.ds(m * TALL, TALL)].astype(jnp.float32))
            totals[t // LANES] = totals[t // LANES] + rows[:8] + rows[8:]
        return tuple(totals)

    totals = (jnp.zeros((8, LANES), jnp.float32),) * (D_EXPERT // LANES)
    for copy, first, count in in_copies(loads, tiled, in_sems):
        copy.wait()
        totals = lax.fori_loop(first, first + count, added, totals)
    means = [jnp.sum(total, axis=0, keepdims=True) / D_MODEL for total in totals]
    scale[...] = jnp.concatenate(means, axis=1)
    factors = [jnp.broadcast_to(1.0 / mean, (TALL, LANES)) for mean in means]
    out_copy = out_copies(ready, held, lambda n: n, out_sems)

    def scaled(n):
        for m, (r, t) in enumerate(tiles):
            rows = tiled[n, pl.ds(m * TALL, TALL)].astype(jnp.float32) * factors[t // LANES]
            held[n, pl.ds(r, TALL), pl.ds(t, LANES)] = rows.astype(jnp.bfloat16)
        out_copy(n).start()

    for_each(scaled)
    for_each(lambda n: out_copy(n).wait())


def up_ready_kernel(at, *refs):
    z, x, c = spot(at)
    own, pieces, (ready, scale, held, in_sems, out_sems) = refs[:4], refs[4:11], refs[11:]
    loads = [(ref.at[pl.ds(z, 1)], n, 1) for n, ref in enumerate(own)]
    loads += [(ref, SIDE * (n + 1), SIDE) for n, ref in enumerate(pieces)]

    def added(n, total):
        for r in range(0, ROWS, TALL):
            rows = jnp.abs(held[n, pl.ds(r, TALL)].astype(jnp.float32))
            total = total + rows[:8] + rows[8:]
        return total

    total = jnp.zeros((8, D_EXPERT), jnp.float32)
    for copy, first, count in in_copies(loads, held, in_sems):
        copy.wait()
        total = lax.fori_loop(first, first + count, added, total)
    mean = jnp.sum(total, axis=0, keepdims=True) / D_MODEL
    scale[...] = mean
    factor = jnp.broadcast_to(1.0 / mean, (TALL, D_EXPERT))

    def slot(n):
        far, near, by_x = (n >> 2) & 3, n & 3, n >> 4
        back_z = (z - jnp.where(by_x == 0, far, near)) & 3
        back_x = (x - jnp.where(by_x == 0, near, far)) & 3
        return back_z * 8 + back_x * 2 + ((c + by_x) & 1)

    out_copy = out_copies(ready, held, slot, out_sems)

    def scaled(n):
        for r in range(0, ROWS, TALL):
            rows = n, pl.ds(r, TALL)
            held[rows] = (held[rows].astype(jnp.float32) * factor).astype(jnp.bfloat16)
        out_copy(n).start()

    for_each(scaled)
    for_each(lambda n: out_copy(n).wait())


def readied(kernel, operands, loads, at=None, tiled=()):
    hbm = pl.BlockSpec(memory_space=pltpu.HBM)
    first = [] if at is None else [pl.BlockSpec(memory_space=pltpu.SMEM)]
    ready, scale = pl.pallas_call(
        kernel,
        in_specs=first + [hbm] * len(operands),
        out_specs=(hbm, pl.BlockSpec(memory_space=pltpu.VMEM)),
        out_shape=(
            jax.ShapeDtypeStruct((D_MODEL, D_EXPERT), jnp.bfloat16),
            jax.ShapeDtypeStruct((1, D_EXPERT), jnp.float32),
        ),
        scratch_shapes=[
            *(pltpu.VMEM(shape, jnp.bfloat16) for shape in tiled),
            pltpu.VMEM((PEERS, ROWS, D_EXPERT), jnp.bfloat16),
            pltpu.SemaphoreType.DMA((loads,)),
            pltpu.SemaphoreType.DMA((PEERS,)),
        ],
    )(*([] if at is None else [at]), *operands)
    return ready[None], scale


def router_kernel(at, *refs):
    pieces, (out, wide) = refs[:4], refs[4:]
    for k, piece in enumerate(pieces):
        base = pl.multiple_of(((at[0] - k) & 3) * 2 * TALL, 2 * TALL)
        for p in range(PEERS // 2):
            left, right = piece[2 * p].astype(jnp.float32), piece[2 * p + 1].astype(jnp.float32)
            cols = pl.ds(p * LANES, LANES)
            low = jnp.concatenate([left[:, :ROWS], right[:, :ROWS]], axis=1)
            high = jnp.concatenate([left[:, ROWS:], right[:, ROWS:]], axis=1)
            wide[pl.ds(base, TALL), cols] = low
            wide[pl.ds(base + TALL, TALL), cols] = high
    for p in range(PEERS // 2):
        cols = pl.ds(p * LANES, LANES)
        out[cols, :] = wide[:, cols].T.astype(jnp.bfloat16)


def router_of(piece):
    pieces = [piece]
    for k in range(1, SIDE):
        pairs = [(y, (y + k) % SIDE) for y in range(SIDE)]
        pieces.append(lax.ppermute(piece, "ep", pairs))
    vmem = pl.BlockSpec(memory_space=pltpu.VMEM)
    return pl.pallas_call(
        router_kernel,
        in_specs=[pl.BlockSpec(memory_space=pltpu.SMEM)] + [vmem] * SIDE,
        out_specs=vmem,
        out_shape=jax.ShapeDtypeStruct((D_MODEL, LANES), jnp.bfloat16),
        scratch_shapes=[pltpu.VMEM((LANES, D_MODEL), jnp.float32)],
        name="router_ready",
    )(lax.axis_index("ep").reshape(1), *pieces)


def shards(train_gate, other_gate, train_up, other_up, router_weight, router_gain):
    at = lax.axis_index("fsdp").reshape(1)
    early_x, early_z = parts_of(at, train_up, other_up, (1, 3))
    late_x, late_z = parts_of(at, train_up, other_up, (2, 0))
    part_x, part_z = early_x | late_x, early_z | late_z
    over_x, over_z = [part_x[0]], [part_z[0]]
    for k in (1, 2, 3):
        over_x.append(moved(part_x[k], 0, k, 0))
        over_z.append(moved(part_z[k], k, 0, 0))
    gate = gate_update(train_gate, other_gate, router_weight, router_gain)
    gate = lax.all_to_all(gate, "fsdp", split_axis=0, concat_axis=0, tiled=True)
    next_z, next_x = regrouped(at, over_x, over_z)
    then_z, then_x = [], []
    for k in range(SIDE):
        then_x.append(moved(next_x[k], 0, k, 1))
        if k:
            then_z.append(moved(next_z[k], k, 0, 0))
    serve_router = router_of(gate[:, TILED:])
    ready_gate, scale_gate = readied(gate_ready_kernel, [gate], 8, tiled=[gate.shape])
    up = [*over_x, *then_z, *then_x]
    ready_up, scale_up = readied(up_ready_kernel, up, 11, at=at)
    return (ready_gate, ready_up, scale_gate, scale_up, serve_router)


def solution(mesh):
    placed = (
        P("ep", "fsdp", None),
        P("ep", "fsdp", None),
        P("ep", "fsdp", None),
        P("ep", "fsdp", None),
        P("fsdp", "ep"),
        P("fsdp"),
    )
    return jax.shard_map(
        shards,
        mesh=mesh,
        in_specs=placed,
        out_specs=(
            P(("ep", "fsdp"), None, None),
            P(("ep", "fsdp"), None, None),
            P(("ep", "fsdp"), None),
            P(("ep", "fsdp"), None),
            P(),
        ),
        check_vma=False,
    )
```
